32 devices in a mesh: dp: 2 (over core), row: 2 (over x), col: 8 (over z, y).
Axes of the slice: x: 2, y: 2, z: 4, core: 2. Of those that a mesh axis runs over, the one named last changes fastest.
Arguments:
- hidden: bfloat16 [512, 28672], P(('dp', 'row'), 'col'), may hold values from -0.25 to 0.25
- upstream: bfloat16 [512, 8192], P('col', ('dp', 'row')), may hold values from -6 to 6
- weight: bfloat16 [28672, 8192], P('col', ('dp', 'row')), may hold values from -0.03125 to 0.03125
Outputs:
- input_grad: bfloat16 [512, 28672], P(('dp', 'row'), 'col')
- weight_grad: float32 [28672, 8192], P('col', ('dp', 'row'))
The draws below stay inside these ranges and needn't reach their ends.
All inputs are finite; a program needn't handle non-finite values.
Results may differ from the reference program's by a relative error of at most 0.014.
Values may be sent and summed in bfloat16 or wider, within the bound.
No kernel may reach another device: no remote copies, remote signals or barrier semaphores. Data moves between devices by JAX's collectives and lax.ppermute only.
A program may use at most 128 MiB of HBM per device.

```python
import jax
import jax.numpy as jnp
from jax import lax

D = 8192
FF = 28672
TOKENS = 512
N_DP = 2
N_ROW = 2


def strengthened(values, rng, source, target, shards_of, factor):
    def block_of(dim):
        return (jnp.arange(values.shape[dim]) // (values.shape[dim] // shards_of)).reshape((-1,) + (1,) * (values.ndim - 1 - dim))

    near = jax.random.permutation(rng, shards_of)[block_of(target)]
    other_side = (block_of(target) + shards_of // 2) % shards_of
    return jnp.where((block_of(source) == near) | (block_of(source) == other_side), factor * values, values)


def steps_of(stream_key, dims, pieces, smallest, high):
    def one(dim, shards_of):
        heights = jax.random.uniform(jax.random.fold_in(jax.random.fold_in(stream_key, 6), dim), (shards_of,), jnp.float32, smallest / len(pieces), high / len(pieces))
        return jnp.repeat(jnp.exp(heights), dims[dim] // shards_of).reshape((-1,) + (1,) * (len(dims) - dim - 1))

    loudness = one(*pieces[0])
    for cut in pieces[1:]:
        loudness = loudness * one(*cut)
    return loudness


def gaussian(key, shape, spread, most, shards=(), kind=jnp.bfloat16):
    drawn = spread * jax.random.normal(key, shape, jnp.float32)
    if shards:
        drawn = drawn * steps_of(key, shape, shards, -0.22, 0.18)
    return jnp.clip(drawn, -most, most).astype(kind)


def bell_draw_with(key, dims, scale, reach, cuts, heavy, dtype=jnp.bfloat16):
    values = scale * jax.random.normal(key, dims, jnp.float32)
    if cuts:
        values = values * steps_of(key, dims, cuts, -0.22, 0.18)
    return jnp.clip(strengthened(values, jax.random.fold_in(key, 3), *heavy), -reach, reach).astype(dtype)


def setup_inputs(seed: int = 0) -> dict:
    arg_keys = jax.random.split(jax.random.key(seed), 4)
    hidden = gaussian(arg_keys[0], (TOKENS, FF), TOKENS ** -0.5, 0.25, ((0, 4), (1, 8)))
    upstream = bell_draw_with(arg_keys[1], (TOKENS, D), 1.0, 6.0, ((0, 8), (1, 4)), (1, 0, 8, 2.0))
    weight = gaussian(arg_keys[2], (FF, D), FF ** -0.5, 0.03125, ((0, 8), (1, 4)))
    return {"hidden": hidden, "upstream": upstream, "weight": weight}


def reference(hidden, upstream, weight):
    weight_grad = lax.dot_general(hidden, upstream, (((0,), (0,)), ((), ())), preferred_element_type=jnp.float32)
    groups = N_DP * N_ROW
    columns = D // groups
    summed = jnp.zeros((hidden.shape[0], FF), jnp.float32)
    for member in range(groups):
        window = upstream[:, member * columns:(member + 1) * columns]
        slab = weight[:, member * columns:(member + 1) * columns]
        product = lax.dot_general(window, slab, (((1,), (1,)), ((), ())), preferred_element_type=jnp.float32)
        rounded = lax.optimization_barrier(product.astype(jnp.bfloat16))
        summed = summed + rounded.astype(jnp.float32)
    return summed.astype(jnp.bfloat16), weight_grad
```

```python
import jax
import jax.numpy as jnp
from jax import lax
from jax.experimental import pallas as pl
from jax.experimental.pallas import tpu as pltpu
from jax.sharding import PartitionSpec as P

TOKENS = ("dp", "row")
ALL = ("dp", "row", "col")


def divisor(n, most):
    fits = [b for b in range(128, most + 1, 128) if n % b == 0]
    return fits[-1] if fits else n


def plain(hidden, upstream, weight):
    gathered = lax.all_gather(upstream, "col", axis=0, tiled=True)
    weight_grad = lax.dot_general(
        lax.all_gather(hidden, TOKENS, axis=0, tiled=True),
        gathered,
        (((0,), (0,)), ((), ())),
        preferred_element_type=jnp.float32,
    )
    summed = lax.psum_scatter(
        lax.dot_general(
            gathered, weight, (((1,), (1,)), ((), ())), preferred_element_type=jnp.float32
        ).astype(jnp.bfloat16),
        TOKENS,
        scatter_dimension=0,
        tiled=True,
    )
    return summed, weight_grad


def block_terms(mine, theirs, weight, name):
    t, d = mine.shape
    ff = weight.shape[0]
    nb = divisor(ff, 896)

    def body(a, b, w, o, u):
        @pl.when(pl.program_id(0) == 0)
        def _():
            y = lax.rem(lax.axis_index("col"), 2)
            u[pl.ds(pl.multiple_of(y * t, t), t), :] = a[...]
            u[pl.ds(pl.multiple_of((1 - y) * t, t), t), :] = b[...]

        o[...] = lax.dot_general(
            u[...], w[...], (((1,), (1,)), ((), ())), preferred_element_type=jnp.float32
        ).astype(o.dtype)

    whole = pl.BlockSpec((t, d), lambda i: (0, 0))
    return pl.pallas_call(
        body,
        grid=(ff // nb,),
        in_specs=[whole, whole, pl.BlockSpec((nb, d), lambda i: (i, 0))],
        out_specs=pl.BlockSpec((2 * t, nb), lambda i: (0, i)),
        out_shape=jax.ShapeDtypeStruct((2 * t, ff), jnp.bfloat16),
        scratch_shapes=[pltpu.VMEM((2 * t, d), jnp.bfloat16)],
        name=name,
        compiler_params=pltpu.CompilerParams(vmem_limit_bytes=24 << 20),
        cost_estimate=pl.CostEstimate(flops=4 * t * d * ff, bytes_accessed=2 * d * ff, transcendentals=0),
    )(mine, theirs, weight)


def weight_gradient(pieces, slots, rows, name):
    t, d = slots[0][0].shape
    m, ff = pieces[0].shape
    n, s = len(pieces), len(slots)
    nb = divisor(ff, 896)

    def body(*refs):
        h, u = refs[:n], refs[n : n + 2 * s]
        o, ups, hid = refs[n + 2 * s :]

        @pl.when(pl.program_id(0) == 0)
        def _():
            c = lax.axis_index("col")
            y, z = lax.rem(c, 2), lax.div(c, 2)
            me = lax.axis_index("dp") * rows + lax.axis_index("row")
            for k in range(s):
                j = lax.bitwise_xor(lax.rem(z + s - k, s), me)
                ups[pl.ds(pl.multiple_of(j * m + y * t, t), t), :] = u[2 * k][...]
                ups[pl.ds(pl.multiple_of(j * m + (1 - y) * t, t), t), :] = u[2 * k + 1][...]

        for j in range(n):
            hid[j * m : (j + 1) * m, :] = h[j][...]
        o[...] = lax.dot_general(
            hid[...], ups[...], (((0,), (0,)), ((), ())), preferred_element_type=jnp.float32
        )

    whole = pl.BlockSpec((t, d), lambda i: (0, 0))
    return pl.pallas_call(
        body,
        grid=(ff // nb,),
        in_specs=[pl.BlockSpec((m, nb), lambda i: (0, i))] * n + [whole] * (2 * s),
        out_specs=pl.BlockSpec((nb, d), lambda i: (i, 0)),
        out_shape=jax.ShapeDtypeStruct((ff, d), jnp.float32),
        scratch_shapes=[pltpu.VMEM((n * m, d), jnp.bfloat16), pltpu.VMEM((n * m, nb), jnp.bfloat16)],
        name=name,
        compiler_params=pltpu.CompilerParams(vmem_limit_bytes=40 << 20),
        cost_estimate=pl.CostEstimate(flops=2 * n * m * d * ff, bytes_accessed=4 * d * ff, transcendentals=0),
    )(*pieces, *[x for pair in slots for x in pair])


def blockwise(shape):
    dps, rows, cols = (shape[a] for a in ALL)
    blocks = dps * rows
    at = lambda d, r, c: (d * rows + r) * cols + c
    swap = [(0, 1), (1, 0)]
    across = [(c, c ^ 1) for c in range(cols)]
    shift = lambda k: [(c, (c + 2 * k) % cols) for c in range(cols)]
    owner = lambda k, c: divmod((c // 2 - k) % blocks, rows)

    def local(hidden, upstream, weight):
        me = lax.axis_index("dp") * rows + lax.axis_index("row")
        far1 = lax.ppermute(upstream, "col", shift(1))
        near0 = lax.ppermute(upstream, "col", across)
        far3 = lax.ppermute(upstream, "col", shift(blocks - 1))
        hidden_x = lax.ppermute(hidden, "row", swap)
        hidden_d = lax.ppermute(hidden, "dp", swap)
        far2 = lax.ppermute(far1, "col", shift(1))
        near1 = lax.ppermute(far1, "col", across)
        near3 = lax.ppermute(far3, "col", across)
        near2 = lax.ppermute(far2, "col", across)
        hidden_xd = lax.ppermute(hidden_x, "dp", swap)
        slots = [(upstream, near0), (far1, near1), (far2, near2), (far3, near3)]

        chip, other = {}, {}
        for k in (0, 1, 3, 2):
            term = block_terms(*slots[k], weight, f"terms{k}")
            to_owner = [
                (at(1 - owner(k, c)[0], r, c), at(owner(k, c)[0], r, c))
                for c in range(cols)
                for r in range(rows)
            ]
            partner = lax.ppermute(term, ALL, to_owner)
            chip[k] = (term.astype(jnp.float32) + partner.astype(jnp.float32)).astype(jnp.bfloat16)
            home = [
                (at(owner(k, c)[0], 1 - owner(k, c)[1], c), at(*owner(k, c), c)) for c in range(cols)
            ]
            other[k] = lax.ppermute(chip[k], ALL, home)
        weight_grad = weight_gradient([hidden, hidden_x, hidden_d, hidden_xd], slots, rows, "wgrad")
        slot = lax.rem(lax.div(lax.axis_index("col"), 2) + blocks - me, blocks)
        own = lax.select_n(slot, *[chip[k] for k in range(blocks)]).astype(jnp.float32)
        for k in range(blocks):
            own = own + other[k].astype(jnp.float32)
        return own.astype(jnp.bfloat16), weight_grad

    return local


def solution(mesh):
    shape = mesh.shape
    fits = shape["dp"] == 2 and shape["row"] == 2 and shape["col"] == 2 * shape["dp"] * shape["row"]
    return jax.shard_map(
        blockwise(shape) if fits else plain,
        mesh=mesh,
        in_specs=(P(TOKENS, "col"), P("col", TOKENS), P("col", TOKENS)),
        out_specs=(P(TOKENS, "col"), P("col", TOKENS)),
        check_vma=False,
    )
```

```python
import jax
import jax.numpy as jnp
from jax import lax
from jax.experimental import pallas as pl
from jax.experimental.pallas import tpu as pltpu
from jax.sharding import PartitionSpec as P


SHARES = (0, 0.3, 0.75, 1)
RING = 4
GRANT_T = 12
GRANT_W = 20
GRANT_S = 6
FETCHES = 4
TOKENS = ("dp", "row")
ALL = ("dp", "row", "col")


def divisor(n, most):
    fits = [b for b in range(128, most + 1, 128) if n % b == 0]
    return fits[-1] if fits else n


def plain(hidden, upstream, weight):
    gathered = lax.all_gather(upstream, "col", axis=0, tiled=True)
    weight_grad = lax.dot_general(
        lax.all_gather(hidden, TOKENS, axis=0, tiled=True),
        gathered,
        (((0,), (0,)), ((), ())),
        preferred_element_type=jnp.float32,
    )
    summed = lax.psum_scatter(
        lax.dot_general(
            gathered, weight, (((1,), (1,)), ((), ())), preferred_element_type=jnp.float32
        ).astype(jnp.bfloat16),
        TOKENS,
        scatter_dimension=0,
        tiled=True,
    )
    return summed, weight_grad


VMEM = pl.BlockSpec(memory_space=pltpu.VMEM)
HBM = pl.BlockSpec(memory_space=pltpu.HBM)


def halves(pieces, ups, t):
    kept = lax.rem(lax.axis_index("col"), 2) == lax.axis_index("dp")
    n = len(pieces) // 2
    first = jnp.where(kept, 0, n * t)
    for i in range(n):
        ups[pl.ds(pl.multiple_of(first + i * t, t), t), :] = pieces[2 * i][...]
        ups[pl.ds(pl.multiple_of(n * t - first + i * t, t), t), :] = pieces[2 * i + 1][...]


def fetched(weight, part):
    ff, d = weight.shape
    half = ff // 2
    cb = half // FETCHES

    def body(w, held, sems):
        def fetch(i):
            return pltpu.make_async_copy(w.at[pl.ds(part * half + i * cb, cb), :], held.at[pl.ds(i * cb, cb), :], sems.at[i])

        for i in range(FETCHES):
            fetch(i).start()
        for i in range(FETCHES):
            fetch(i).wait()

    return pl.pallas_call(
        body,
        in_specs=[HBM],
        out_specs=VMEM,
        out_shape=jax.ShapeDtypeStruct((half, d), weight.dtype),
        scratch_shapes=[pltpu.SemaphoreType.DMA((FETCHES,))],
        compiler_params=pltpu.CompilerParams(vmem_limit_bytes=GRANT_S << 20),
        cost_estimate=pl.CostEstimate(flops=d * half, bytes_accessed=2 * d * half, transcendentals=0),
    )(pltpu.with_memory_space_constraint(weight, pltpu.HBM))


def block_terms(slots, weights):
    t, d = slots[0][0].shape
    half = weights[0].shape[0]
    n = len(slots)
    cb = divisor(half, 896)
    steps = half // cb

    def body(*refs):
        u, w = refs[: 2 * n], refs[2 * n : 2 * n + 2]
        keep, give, ups = refs[2 * n + 2 :]
        halves(u, ups, t)
        for h in range(2):

            def step(i, carry):
                term = lax.dot_general(
                    ups[...],
                    w[h][pl.ds(pl.multiple_of(i * cb, cb), cb), :],
                    (((1,), (1,)), ((), ())),
                    preferred_element_type=jnp.float32,
                ).astype(jnp.bfloat16)
                here = pl.ds(pl.multiple_of(h * half + i * cb, cb), cb)
                keep[:, here] = term[: n * t]
                give[:, here] = term[n * t :]
                return carry

            lax.fori_loop(0, steps, step, 0)

    out = jax.ShapeDtypeStruct((n * t, 2 * half), jnp.bfloat16)
    return pl.pallas_call(
        body,
        in_specs=[VMEM] * (2 * n + 2),
        out_specs=[VMEM] * 2,
        out_shape=[out, out],
        scratch_shapes=[pltpu.VMEM((2 * n * t, d), jnp.bfloat16)],
        compiler_params=pltpu.CompilerParams(vmem_limit_bytes=GRANT_T << 20),
        cost_estimate=pl.CostEstimate(flops=8 * n * t * d * half, bytes_accessed=4 * d * half, transcendentals=0),
    )(*[x for pair in slots for x in pair], *weights)


def weight_gradient(pieces, ups, rows, part, into):
    first = part == 0
    slots = ups if first else []
    t, d = slots[0][0].shape if first else (ups.shape[0] // 8, ups.shape[1])
    m, ff = pieces[0].shape
    n, s = len(pieces), len(slots)
    cb = divisor(ff, 256)
    steps = ff // cb
    lo, hi = round(steps * SHARES[part]), round(steps * SHARES[part + 1])
    ring = min(RING, hi - lo)
    operands = list(pieces) + ([x for pair in slots for x in pair] if first else [ups, into])

    def body(*refs):
        h, u = refs[:n], refs[n : n + 2 * s] if first else refs[n]
        rest = refs[len(operands) :]
        if first:
            o, ups_ref, out, sent = rest
            c = lax.axis_index("col")
            y, z = lax.rem(c, 2), lax.div(c, 2)
            me = lax.axis_index("dp") * rows + lax.axis_index("row")
            for k in range(s):
                j = lax.bitwise_xor(lax.rem(z + s - k, s), me)
                ups_ref[pl.ds(pl.multiple_of(j * m + y * t, t), t), :] = u[2 * k][...]
                ups_ref[pl.ds(pl.multiple_of(j * m + (1 - y) * t, t), t), :] = u[2 * k + 1][...]
        else:
            o, out, sent = rest
            ups_ref = u

        def store(i):
            slot = lax.rem(i - lo, ring)
            return pltpu.make_async_copy(
                out.at[slot], o.at[pl.ds(pl.multiple_of(i * cb, cb), cb), :], sent.at[slot]
            )

        def step(i, carry):
            @pl.when(i >= lo + ring)
            def _():
                store(i - ring).wait()

            here = pl.ds(pl.multiple_of(i * cb, cb), cb)
            hid = jnp.concatenate([x[:, here] for x in h], axis=0)
            out[lax.rem(i - lo, ring)] = lax.dot_general(
                hid, ups_ref[...], (((0,), (0,)), ((), ())), preferred_element_type=jnp.float32
            )
            store(i).start()
            return carry

        lax.fori_loop(lo, hi, step, 0)
        for i in range(hi - ring, hi):
            store(jnp.int32(i)).wait()

    width = (hi - lo) * cb
    grad = jax.ShapeDtypeStruct((ff, d), jnp.float32)
    everyone = jax.ShapeDtypeStruct((n * m, d), jnp.bfloat16)
    return pl.pallas_call(
        body,
        in_specs=[VMEM] * n + ([VMEM] * (2 * s) if first else [VMEM, HBM]),
        out_specs=[HBM, VMEM] if first else [HBM],
        out_shape=[grad, everyone] if first else [grad],
        input_output_aliases={} if first else {len(operands) - 1: 0},
        scratch_shapes=[pltpu.VMEM((ring, cb, d), jnp.float32), pltpu.SemaphoreType.DMA((ring,))],
        compiler_params=pltpu.CompilerParams(vmem_limit_bytes=GRANT_W << 20),
        cost_estimate=pl.CostEstimate(flops=2 * n * m * d * width, bytes_accessed=4 * d * width, transcendentals=0),
    )(*operands)


def small(body, outs, *args):
    return pl.pallas_call(
        body,
        in_specs=[VMEM] * len(args),
        out_specs=[VMEM] * len(outs),
        out_shape=[jax.ShapeDtypeStruct(o, jnp.bfloat16) for o in outs],
        compiler_params=pltpu.CompilerParams(vmem_limit_bytes=GRANT_S << 20),
        cost_estimate=pl.CostEstimate(flops=2 * args[0].size, bytes_accessed=8 * args[0].size, transcendentals=0),
    )(*args)


def even_is_home(rows):
    return lax.rem(lax.div(lax.axis_index("col"), 2), rows) == lax.axis_index("row")


def wide(x):
    return x.astype(jnp.float32)


def chip_sums(keep, got, rows):
    t = keep.shape[0] // 2

    def body(keep, got, stay, go):
        first = jnp.where(even_is_home(rows), 0, t)
        for out, start in ((stay, first), (go, t - first)):
            at = pl.ds(pl.multiple_of(start, t), t)
            out[...] = (wide(keep[at, :]) + wide(got[at, :])).astype(out.dtype)

    return small(body, [(t, keep.shape[1])] * 2, keep, got)


def finish(stay_a, come_a, stay_b, come_b, rows, blocks):
    def body(stay_a, come_a, stay_b, come_b, kept, give):
        z = lax.div(lax.axis_index("col"), 2)
        slot = jnp.where(even_is_home(rows), 0, 1)
        mine = lax.div(lax.rem(z + blocks - slot, blocks), rows) == lax.axis_index("dp")

        @pl.when(mine)
        def _():
            kept[...] = (wide(stay_a[...]) + wide(come_a[...])).astype(kept.dtype)
            give[...] = (wide(stay_b[...]) + wide(come_b[...])).astype(give.dtype)

        @pl.when(jnp.logical_not(mine))
        def _():
            give[...] = (wide(stay_a[...]) + wide(come_a[...])).astype(kept.dtype)
            kept[...] = (wide(stay_b[...]) + wide(come_b[...])).astype(give.dtype)

    return small(body, [stay_a.shape] * 2, stay_a, come_a, stay_b, come_b)


def joined(kept, got):
    t = kept.shape[0]

    def body(kept, got, o):
        core = lax.axis_index("dp")
        o[pl.ds(pl.multiple_of(core * t, t), t), :] = kept[...]
        o[pl.ds(pl.multiple_of((1 - core) * t, t), t), :] = got[...]

    return small(body, [(2 * t, kept.shape[1])], kept, got)[0]


def blockwise(shape):
    dps, rows, cols = (shape[a] for a in ALL)
    blocks = dps * rows
    swap = [(0, 1), (1, 0)]
    across = [(c, c ^ 1) for c in range(cols)]
    shift = lambda k: [(c, (c + 2 * k) % cols) for c in range(cols)]
    move = lambda x, axis, perm: lax.ppermute(x, axis, perm)

    def local(hidden, upstream, weight):
        far1 = move(upstream, "col", shift(1))
        near0 = move(upstream, "col", across)
        far3 = move(upstream, "col", shift(blocks - 1))
        hidden_x = move(hidden, "row", swap)
        hidden_d = move(hidden, "dp", swap)
        near1 = move(far1, "col", across)
        far2 = move(far1, "col", shift(1))
        near3 = move(far3, "col", across)
        near2 = move(far2, "col", across)
        hidden_xd = move(hidden_x, "dp", swap)
        slots = [(upstream, near0), (far1, near1), (far2, near2), (far3, near3)]
        pieces = [hidden, hidden_x, hidden_d, hidden_xd]

        held = [fetched(weight, i) for i in range(2)]
        keep_a, give_a = block_terms([slots[0], slots[1]], held)
        got_a = move(give_a, "dp", swap)
        stay_a, go_a = chip_sums(keep_a, got_a, rows)
        come_a = move(go_a, "row", swap)
        keep_b, give_b = block_terms([slots[2], slots[3]], held)
        got_b = move(give_b, "dp", swap)
        grad, ups = weight_gradient(pieces, slots, rows, 0, None)
        stay_b, go_b = chip_sums(keep_b, got_b, rows)
        come_b = move(go_b, "row", swap)
        grad, = weight_gradient(pieces, ups, rows, 1, grad)
        kept, give = finish(stay_a, come_a, stay_b, come_b, rows, blocks)
        got = move(give, "dp", swap)
        for p in range(2, len(SHARES) - 1):
            grad, = weight_gradient(pieces, ups, rows, p, grad)
        return joined(kept, got), grad

    return local


def solution(mesh):
    shape = mesh.shape
    fits = shape["dp"] == 2 and shape["row"] == 2 and shape["col"] == 2 * shape["dp"] * shape["row"]
    return jax.shard_map(
        blockwise(shape) if fits else plain,
        mesh=mesh,
        in_specs=(P(TOKENS, "col"), P("col", TOKENS), P("col", TOKENS)),
        out_specs=(P(TOKENS, "col"), P("col", TOKENS)),
        check_vma=False,
    )
```

```python
import jax
import jax.numpy as jnp
from jax import lax
from jax.experimental import pallas as pl
from jax.experimental.pallas import tpu as pltpu
from jax.sharding import PartitionSpec as P


SHARES = (0, 0.929, 1)
RING = 6
GRANT_T = 16
GRANT_W = 24
GRANT_S = 6
FETCHES = 4
TOKENS = ("dp", "row")
ALL = ("dp", "row", "col")


def divisor(n, most):
    fits = [b for b in range(128, most + 1, 128) if n % b == 0]
    return fits[-1] if fits else n


def plain(hidden, upstream, weight):
    gathered = lax.all_gather(upstream, "col", axis=0, tiled=True)
    weight_grad = lax.dot_general(
        lax.all_gather(hidden, TOKENS, axis=0, tiled=True),
        gathered,
        (((0,), (0,)), ((), ())),
        preferred_element_type=jnp.float32,
    )
    summed = lax.psum_scatter(
        lax.dot_general(
            gathered, weight, (((1,), (1,)), ((), ())), preferred_element_type=jnp.float32
        ).astype(jnp.bfloat16),
        TOKENS,
        scatter_dimension=0,
        tiled=True,
    )
    return summed, weight_grad


VMEM = pl.BlockSpec(memory_space=pltpu.VMEM)
HBM = pl.BlockSpec(memory_space=pltpu.HBM)


def halves(pieces, ups, t):
    kept = lax.rem(lax.axis_index("col"), 2) == lax.axis_index("dp")
    n = len(pieces) // 2
    first = jnp.where(kept, 0, n * t)
    for i in range(n):
        ups[pl.ds(pl.multiple_of(first + i * t, t), t), :] = pieces[2 * i][...]
        ups[pl.ds(pl.multiple_of(n * t - first + i * t, t), t), :] = pieces[2 * i + 1][...]


def fetched(weight, part):
    ff, d = weight.shape
    half = ff // 2
    cb = half // FETCHES

    def body(w, held, sems):
        def fetch(i):
            return pltpu.make_async_copy(w.at[pl.ds(part * half + i * cb, cb), :], held.at[pl.ds(i * cb, cb), :], sems.at[i])

        for i in range(FETCHES):
            fetch(i).start()
        for i in range(FETCHES):
            fetch(i).wait()

    return pl.pallas_call(
        body,
        in_specs=[HBM],
        out_specs=VMEM,
        out_shape=jax.ShapeDtypeStruct((half, d), weight.dtype),
        scratch_shapes=[pltpu.SemaphoreType.DMA((FETCHES,))],
        compiler_params=pltpu.CompilerParams(vmem_limit_bytes=GRANT_S << 20),
        cost_estimate=pl.CostEstimate(flops=d * half, bytes_accessed=2 * d * half, transcendentals=0),
    )(pltpu.with_memory_space_constraint(weight, pltpu.HBM))


def block_terms(slots, weights):
    t, d = slots[0][0].shape
    half = weights[0].shape[0]
    n, parts = len(slots), len(weights)
    cb = divisor(half, 1792)
    steps = half // cb

    def body(*refs):
        u, w = refs[: 2 * n], refs[2 * n : 2 * n + parts]
        keep, give, ups = refs[2 * n + parts :]
        halves(u, ups, t)
        for h in range(parts):

            def step(i, carry):
                term = lax.dot_general(
                    ups[...],
                    w[h][pl.ds(pl.multiple_of(i * cb, cb), cb), :],
                    (((1,), (1,)), ((), ())),
                    preferred_element_type=jnp.float32,
                ).astype(jnp.bfloat16)
                here = pl.ds(pl.multiple_of(h * half + i * cb, cb), cb)
                keep[:, here] = term[: n * t]
                give[:, here] = term[n * t :]
                return carry

            lax.fori_loop(0, steps, step, 0)

    out = jax.ShapeDtypeStruct((n * t, parts * half), jnp.bfloat16)
    return pl.pallas_call(
        body,
        in_specs=[VMEM] * (2 * n + parts),
        out_specs=[VMEM] * 2,
        out_shape=[out, out],
        scratch_shapes=[pltpu.VMEM((2 * n * t, d), jnp.bfloat16)],
        compiler_params=pltpu.CompilerParams(vmem_limit_bytes=GRANT_T << 20),
        cost_estimate=pl.CostEstimate(flops=4 * n * t * d * half * parts, bytes_accessed=2 * d * half * parts, transcendentals=0),
    )(*[x for pair in slots for x in pair], *weights)


def weight_gradient(pieces, ups, rows, part, into):
    first = part == 0
    slots = ups if first else []
    t, d = slots[0][0].shape if first else (ups.shape[0] // 8, ups.shape[1])
    m, ff = pieces[0].shape
    n, s = len(pieces), len(slots)
    cb = divisor(ff, 256)
    steps = ff // cb
    lo, hi = round(steps * SHARES[part]), round(steps * SHARES[part + 1])
    ring = min(RING, hi - lo)
    operands = list(pieces) + ([x for pair in slots for x in pair] if first else [ups, into])

    def body(*refs):
        h, u = refs[:n], refs[n : n + 2 * s] if first else refs[n]
        rest = refs[len(operands) :]
        if first:
            o, ups_ref, out, sent = rest
            c = lax.axis_index("col")
            y, z = lax.rem(c, 2), lax.div(c, 2)
            me = lax.axis_index("dp") * rows + lax.axis_index("row")
            for k in range(s):
                j = lax.bitwise_xor(lax.rem(z + s - k, s), me)
                ups_ref[pl.ds(pl.multiple_of(j * m + y * t, t), t), :] = u[2 * k][...]
                ups_ref[pl.ds(pl.multiple_of(j * m + (1 - y) * t, t), t), :] = u[2 * k + 1][...]
        else:
            o, out, sent = rest
            ups_ref = u

        def store(i):
            slot = (i - lo) % ring
            return pltpu.make_async_copy(
                out.at[slot], o.at[pl.ds(i * cb, cb), :], sent.at[slot]
            )

        def step(i, carry):
            if i >= lo + ring:
                store(i - ring).wait()

            here = pl.ds(i * cb, cb)
            hid = jnp.concatenate([x[:, here] for x in h], axis=0)
            out[(i - lo) % ring] = lax.dot_general(
                hid, ups_ref[...], (((0,), (0,)), ((), ())), preferred_element_type=jnp.float32
            )
            store(i).start()
            return carry

        for i in range(lo, hi):
            step(i, 0)
        for i in range(hi - ring, hi):
            store(i).wait()

    width = (hi - lo) * cb
    grad = jax.ShapeDtypeStruct((ff, d), jnp.float32)
    everyone = jax.ShapeDtypeStruct((n * m, d), jnp.bfloat16)
    return pl.pallas_call(
        body,
        in_specs=[VMEM] * n + ([VMEM] * (2 * s) if first else [VMEM, HBM]),
        out_specs=[HBM, VMEM] if first else [HBM],
        out_shape=[grad, everyone] if first else [grad],
        input_output_aliases={} if first else {len(operands) - 1: 0},
        scratch_shapes=[pltpu.VMEM((ring, cb, d), jnp.float32), pltpu.SemaphoreType.DMA((ring,))],
        compiler_params=pltpu.CompilerParams(vmem_limit_bytes=GRANT_W << 20),
        cost_estimate=pl.CostEstimate(flops=2 * n * m * d * width, bytes_accessed=4 * d * width, transcendentals=0),
    )(*operands)


def small(body, outs, *args):
    return pl.pallas_call(
        body,
        in_specs=[VMEM] * len(args),
        out_specs=[VMEM] * len(outs),
        out_shape=[jax.ShapeDtypeStruct(o, jnp.bfloat16) for o in outs],
        compiler_params=pltpu.CompilerParams(vmem_limit_bytes=GRANT_S << 20),
        cost_estimate=pl.CostEstimate(flops=2 * args[0].size, bytes_accessed=8 * args[0].size, transcendentals=0),
    )(*args)


def even_is_home(rows):
    return lax.rem(lax.div(lax.axis_index("col"), 2), rows) == lax.axis_index("row")


def wide(x):
    return x.astype(jnp.float32)


def chip_sums(keep, got, rows):
    t = keep.shape[0] // 2

    def body(keep, got, stay, go):
        first = jnp.where(even_is_home(rows), 0, t)
        for out, start in ((stay, first), (go, t - first)):
            at = pl.ds(pl.multiple_of(start, t), t)
            out[...] = (wide(keep[at, :]) + wide(got[at, :])).astype(out.dtype)

    return small(body, [(t, keep.shape[1])] * 2, keep, got)


def finish(stay_a, come_a, stay_b, come_b, rows, blocks):
    sizes = [len(stay_a), len(stay_b)]

    def body(*refs):
        kept, give = refs[-2:]
        z = lax.div(lax.axis_index("col"), 2)
        slot = jnp.where(even_is_home(rows), 0, 1)
        mine = lax.div(lax.rem(z + blocks - slot, blocks), rows) == lax.axis_index("dp")

        def fill(out, parts):
            at = 0
            for i in range(len(parts) // 2):
                width = parts[i].shape[1]
                total = wide(parts[i][...]) + wide(parts[i + len(parts) // 2][...])
                out[:, at : at + width] = total.astype(out.dtype)
                at += width

        a, b = refs[: 2 * sizes[0]], refs[2 * sizes[0] : -2]

        @pl.when(mine)
        def _():
            fill(kept, a)
            fill(give, b)

        @pl.when(jnp.logical_not(mine))
        def _():
            fill(give, a)
            fill(kept, b)

    shape = (stay_a[0].shape[0], sum(x.shape[1] for x in stay_a))
    return small(body, [shape] * 2, *stay_a, *come_a, *stay_b, *come_b)


def joined(kept, got):
    t = kept.shape[0]

    def body(kept, got, o):
        core = lax.axis_index("dp")
        o[pl.ds(pl.multiple_of(core * t, t), t), :] = kept[...]
        o[pl.ds(pl.multiple_of((1 - core) * t, t), t), :] = got[...]

    return small(body, [(2 * t, kept.shape[1])], kept, got)[0]


def blockwise(shape):
    dps, rows, cols = (shape[a] for a in ALL)
    blocks = dps * rows
    swap = [(0, 1), (1, 0)]
    across = [(c, c ^ 1) for c in range(cols)]
    shift = lambda k: [(c, (c + 2 * k) % cols) for c in range(cols)]
    move = lambda x, axis, perm: lax.ppermute(x, axis, perm)

    def local(hidden, upstream, weight):
        far1 = move(upstream, "col", shift(1))
        near0 = move(upstream, "col", across)
        far3 = move(upstream, "col", shift(blocks - 1))
        hidden_x = move(hidden, "row", swap)
        hidden_d = move(hidden, "dp", swap)
        near1 = move(far1, "col", across)
        far2 = move(far1, "col", shift(1))
        near3 = move(far3, "col", across)
        near2 = move(near1, "col", shift(1))
        hidden_xd = move(hidden_x, "dp", swap)
        slots = [(upstream, near0), (far1, near1), (far2, near2), (far3, near3)]
        pieces = [hidden, hidden_x, hidden_d, hidden_xd]

        held = [fetched(weight, i) for i in range(2)]

        def exchanged(pair):
            stay, come, keeps, gots = [], [], [], []
            for i in range(2):
                keep, give = block_terms(pair, held[i : i + 1])
                keeps.append(keep)
                gots.append(move(give, "dp", swap))
            for i in range(2):
                near, go = chip_sums(keeps[i], gots[i], rows)
                stay.append(near)
                come.append(move(go, "row", swap))
            return stay, come

        stay_a, come_a = exchanged([slots[0], slots[1]])
        stay_b, come_b = exchanged([slots[2], slots[3]])
        grad, ups = weight_gradient(pieces, slots, rows, 0, None)
        kept, give = finish(stay_a, come_a, stay_b, come_b, rows, blocks)
        got = move(give, "dp", swap)
        for p in range(1, len(SHARES) - 1):
            grad, = weight_gradient(pieces, ups, rows, p, grad)
        return joined(kept, got), grad

    return local


def solution(mesh):
    shape = mesh.shape
    fits = shape["dp"] == 2 and shape["row"] == 2 and shape["col"] == 2 * shape["dp"] * shape["row"]
    return jax.shard_map(
        blockwise(shape) if fits else plain,
        mesh=mesh,
        in_specs=(P(TOKENS, "col"), P("col", TOKENS), P("col", TOKENS)),
        out_specs=(P(TOKENS, "col"), P("col", TOKENS)),
        check_vma=False,
    )
```
